32 devices in a mesh: seq: 8 (over y, x, core), head: 4 (over z).
Axes of the slice: x: 2, y: 2, z: 4, core: 2. Of those that a mesh axis runs over, the one named last changes fastest.
Arguments:
- query_rows: bfloat16 [1024, 2048], P('seq', 'head'), may hold values from -6 to 6
- key_rows: bfloat16 [1024, 128], P('seq'), may hold values from -6 to 6
- value_rows: bfloat16 [1024, 128], P('seq'), may hold values from -6 to 6
- out_grad: bfloat16 [1024, 2048], P('seq', 'head'), may hold values from -3 to 3
Outputs:
- attended: bfloat16 [1024, 2048], P('seq', 'head')
- query_grad: bfloat16 [1024, 2048], P('seq', 'head')
- key_grad: bfloat16 [1024, 128], P('seq')
- value_grad: bfloat16 [1024, 128], P('seq')
The draws below stay inside these ranges and needn't reach their ends.
All inputs are finite; a program needn't handle non-finite values.
Results may differ from the reference program's by a relative error of at most 0.023.
Values may be sent and summed in bfloat16 or wider, within the bound.
No kernel may reach another device: no remote copies, remote signals or barrier semaphores. Data moves between devices by JAX's collectives and lax.ppermute only.
A program may use at most 64 MiB of HBM per device.

```python
import jax
import jax.numpy as jnp
import numpy as np
from jax import lax

D = 128
H = 16
TOK_DEV = 128
FEAT = 8256
TOKENS = 1024


def block_scale(own_key, extent, split, low, top_value):
    loudness, own = 1.0, jax.random.fold_in(own_key, 6)
    for position, blocks in split:
        draws = jnp.exp(jax.random.uniform(jax.random.fold_in(own, position), (blocks,), jnp.float32, low / len(split), top_value / len(split)))
        loudness = loudness * jnp.repeat(draws, extent[position] // blocks).reshape([-1 if axis == position else 1 for axis in range(len(extent))])
    return loudness


def bell_draw(stream_key, shape, deviation, limit, shards=(), kind=jnp.bfloat16):
    level = block_scale(stream_key, shape, shards, -0.22, 0.18) if shards else 1.0
    array = jax.random.normal(stream_key, shape, jnp.float32) * deviation * level
    return jnp.minimum(jnp.maximum(array, -limit), limit).astype(kind)


def setup_inputs(seed: int = 0) -> dict:
    streams_of = jax.random.split(jax.random.key(seed), 5)
    query_rows = bell_draw(streams_of[0], (TOKENS, H * D), 1.0, 6.0, ((0, 8), (1, 4)))
    key_rows = bell_draw(streams_of[1], (TOKENS, D), 1.0, 6.0, ((0, 8),))
    value_rows = bell_draw(streams_of[2], (TOKENS, D), 1.0, 6.0, ((0, 8),))
    out_grad = bell_draw(streams_of[3], (TOKENS, H * D), 0.5, 3.0, ((0, 8), (1, 4)))
    return {"query_rows": query_rows, "key_rows": key_rows, "value_rows": value_rows, "out_grad": out_grad}


EPSILON = 1e-06

def pair_tables(head_width):
    first_index, second_index = np.triu_indices(head_width)
    return (jnp.asarray(first_index, dtype=jnp.int32), jnp.asarray(second_index, dtype=jnp.int32))

def rounded(quantity):
    return lax.optimization_barrier(quantity.astype(jnp.bfloat16)).astype(jnp.float32)

def expand(source, first_index, second_index):
    return jnp.take(source, first_index, axis=-1) * jnp.take(source, second_index, axis=-1)

def spread_back(coeffs, source, first_index, second_index, head_width):
    left_terms = rounded(coeffs * jnp.take(source, second_index, axis=-1))
    right_terms = rounded(coeffs * jnp.take(source, first_index, axis=-1))
    summed = jax.ops.segment_sum(left_terms.T, first_index, num_segments=head_width)
    summed = summed + jax.ops.segment_sum(right_terms.T, second_index, num_segments=head_width)
    return summed.T

def reference(query_rows, key_rows, value_rows, out_grad):
    first_index, second_index = pair_tables(D)
    multiplicity = jnp.where(first_index == second_index, 1.0, 2.0).astype(jnp.float32)
    blocks = TOKENS // TOK_DEV
    query_blocks = query_rows.reshape(blocks, TOK_DEV, H, D).transpose(0, 2, 1, 3)
    grad_blocks = out_grad.reshape(blocks, TOK_DEV, H, D).transpose(0, 2, 1, 3)
    key_blocks = key_rows.reshape(blocks, TOK_DEV, D)
    value_blocks = value_rows.reshape(blocks, TOK_DEV, D)
    places = jnp.arange(TOK_DEV, dtype=jnp.int32)
    causal = places[:, None] >= places[None, :]

    def forward_block(running, inputs):
        query_block, grad_block, key_block, value_block = inputs
        prefix = rounded(running)
        key_float = key_block.astype(jnp.float32)
        value_float = value_block.astype(jnp.float32)

        def per_head(carried, head_pair):
            query_head, grad_head = head_pair
            query_float = query_head.astype(jnp.float32)
            products = jnp.dot(query_float, key_float.T, preferred_element_type=jnp.float32)
            weights = rounded(jnp.where(causal, products * products, 0.0))
            features = rounded(expand(query_float, first_index, second_index) * multiplicity)
            numerator = jnp.dot(weights, value_float, preferred_element_type=jnp.float32)
            numerator = numerator + jnp.dot(features, prefix, preferred_element_type=jnp.float32)
            root_mean = jnp.sqrt(lax.optimization_barrier(jnp.mean(numerator * numerator, axis=-1, keepdims=True)) + EPSILON)
            normed = numerator / root_mean
            grad_float = grad_head.astype(jnp.float32)
            numer_grad = rounded((grad_float - normed * lax.optimization_barrier(jnp.mean(grad_float * normed, axis=-1, keepdims=True))) / root_mean)
            value_dots = jnp.dot(numer_grad, value_float.T, preferred_element_type=jnp.float32)
            coefficient = rounded(jnp.where(causal, 2.0 * products * value_dots, 0.0))
            query_part = jnp.dot(numer_grad, prefix.T, preferred_element_type=jnp.float32) * multiplicity
            query_grad = jnp.dot(coefficient, key_float, preferred_element_type=jnp.float32)
            query_grad = query_grad + spread_back(query_part, query_float, first_index, second_index, D)
            dual_sum, key_sum, value_sum = carried
            dual_sum = dual_sum + jnp.dot(features.T, numer_grad, preferred_element_type=jnp.float32)
            key_sum = key_sum + jnp.dot(coefficient.T, query_float, preferred_element_type=jnp.float32)
            value_sum = value_sum + jnp.dot(weights.T, numer_grad, preferred_element_type=jnp.float32)
            return ((dual_sum, key_sum, value_sum), (normed.astype(jnp.bfloat16), query_grad.astype(jnp.bfloat16)))
        initial = (jnp.zeros((FEAT, D), jnp.float32), jnp.zeros((TOK_DEV, D), jnp.float32), jnp.zeros((TOK_DEV, D), jnp.float32))
        sums, outputs = lax.scan(per_head, initial, (query_block, grad_block))
        key_features = rounded(expand(key_float, first_index, second_index))
        running = running + jnp.dot(key_features.T, value_float, preferred_element_type=jnp.float32)
        return (running, (outputs[0], outputs[1], sums[0], sums[1], sums[2]))
    start_state = jnp.zeros((FEAT, D), jnp.float32)
    final_state, forward_out = lax.scan(forward_block, start_state, (query_blocks, grad_blocks, key_blocks, value_blocks))
    attended_blocks, query_grad_blocks, duals, key_sums, value_sums = forward_out

    def backward_block(running, inputs):
        dual_term, key_block, value_block, key_sum, value_sum = inputs
        suffix = rounded(running)
        key_float = key_block.astype(jnp.float32)
        value_float = value_block.astype(jnp.float32)
        key_features = rounded(expand(key_float, first_index, second_index))
        key_part = jnp.dot(value_float, suffix.T, preferred_element_type=jnp.float32)
        key_grad = key_sum + spread_back(key_part, key_float, first_index, second_index, D)
        value_grad = value_sum + jnp.dot(key_features, suffix, preferred_element_type=jnp.float32)
        return (running + dual_term, (key_grad.astype(jnp.bfloat16), value_grad.astype(jnp.bfloat16)))
    final_dual, backward_out = lax.scan(backward_block, start_state, (duals, key_blocks, value_blocks, key_sums, value_sums), reverse=True)
    attended = attended_blocks.transpose(0, 2, 1, 3).reshape(TOKENS, H * D)
    query_grad = query_grad_blocks.transpose(0, 2, 1, 3).reshape(TOKENS, H * D)
    key_grad = backward_out[0].reshape(TOKENS, D)
    value_grad = backward_out[1].reshape(TOKENS, D)
    return (attended, query_grad, key_grad, value_grad)
```

```python
import functools

import jax
import jax.numpy as jnp
from jax import lax
from jax.experimental import pallas as pl
from jax.experimental.pallas import tpu as pltpu
from jax.sharding import PartitionSpec as P

EPSILON = 1e-06


def contract(left, right, left_dim, right_dim):
    return lax.dot_general(
        left, right, (((left_dim,), (right_dim,)), ((), ())), preferred_element_type=jnp.float32
    )


def attention_kernel(
    key_ref, value_ref, query_ref, grad_ref, out_ref, dquery_ref, dkv_ref, score_ref, weight_ref
):
    rows, width = query_ref.shape
    tokens, head_width = key_ref.shape
    heads = width // head_width
    chunk = min(tokens, 2 * rows)
    start = lax.axis_index("seq") * rows

    def stacked(ref):
        return jnp.concatenate(
            [ref[:, h * head_width : (h + 1) * head_width] for h in range(heads)], axis=0
        )

    query = stacked(query_ref)
    key_place = lax.broadcasted_iota(jnp.int32, (chunk, heads * rows), 0)
    query_place = lax.broadcasted_iota(jnp.int32, (chunk, heads * rows), 1) % rows
    ahead = key_place - query_place
    numerator = jnp.zeros((head_width, heads * rows), jnp.float32)
    for at in range(0, tokens, chunk):
        part = slice(at, at + chunk)
        score = contract(key_ref[part, :], query, 1, 1)
        score = jnp.where(ahead <= start - at, score, 0.0)
        weight = (score * score).astype(jnp.bfloat16)
        score_ref[part, :] = score
        weight_ref[part, :] = weight
        numerator = numerator + contract(value_ref[part, :], weight, 0, 0)
    numerator = numerator.T
    root_mean = jnp.sqrt(jnp.mean(numerator * numerator, axis=-1, keepdims=True) + EPSILON)
    normed = numerator / root_mean
    grad = stacked(grad_ref).astype(jnp.float32)
    numer_grad = (
        (grad - normed * jnp.mean(grad * normed, axis=-1, keepdims=True)) / root_mean
    ).astype(jnp.bfloat16)
    attended = normed.astype(jnp.bfloat16)
    dquery = jnp.zeros((head_width, heads * rows), jnp.float32)
    for at in range(0, tokens, chunk):
        part = slice(at, at + chunk)
        value_dots = contract(value_ref[part, :], numer_grad, 1, 1)
        coefficient = (2.0 * score_ref[part, :] * value_dots).astype(jnp.bfloat16)
        dquery = dquery + contract(key_ref[part, :], coefficient, 0, 0)
        dkv_ref[part, :head_width] = contract(coefficient, query, 1, 0).astype(jnp.bfloat16)
        dkv_ref[part, head_width:] = contract(weight_ref[part, :], numer_grad, 1, 0).astype(
            jnp.bfloat16
        )
    dquery = dquery.T.astype(jnp.bfloat16)
    for h in range(heads):
        cols = slice(h * head_width, (h + 1) * head_width)
        out_ref[:, cols] = attended[h * rows : (h + 1) * rows, :]
        dquery_ref[:, cols] = dquery[h * rows : (h + 1) * rows, :]


def local(query_rows, key_rows, value_rows, out_grad):
    rows, head_width = key_rows.shape
    blocks, head_axis = lax.axis_size("seq"), lax.axis_size("head")
    tokens = rows * blocks
    columns = query_rows.shape[1] // head_width * rows
    keys = lax.all_gather(key_rows, "seq", axis=0, tiled=True)
    values = lax.all_gather(value_rows, "seq", axis=0, tiled=True)
    vmem = pl.BlockSpec(memory_space=pltpu.VMEM)
    attended, query_grad, partial = pl.pallas_call(
        attention_kernel,
        out_shape=(
            jax.ShapeDtypeStruct(query_rows.shape, jnp.bfloat16),
            jax.ShapeDtypeStruct(query_rows.shape, jnp.bfloat16),
            jax.ShapeDtypeStruct((tokens, 2 * head_width), jnp.bfloat16),
        ),
        in_specs=[vmem] * 4,
        out_specs=(vmem,) * 3,
        scratch_shapes=[
            pltpu.VMEM((tokens, columns), jnp.float32),
            pltpu.VMEM((tokens, columns), jnp.bfloat16),
        ],
        name="attention",
    )(keys, values, query_rows, out_grad)
    pieces = lax.all_to_all(partial.reshape(blocks, rows, 2 * head_width), "seq", 0, 0)
    summed = jnp.sum(pieces.astype(jnp.float32), axis=0)
    sent = summed.astype(jnp.bfloat16)
    for step in range(1, head_axis):
        ring = [(i, (i + step) % head_axis) for i in range(head_axis)]
        summed = summed + lax.ppermute(sent, "head", ring).astype(jnp.float32)
    summed = summed.astype(jnp.bfloat16)
    return (attended, query_grad, summed[:, :head_width], summed[:, head_width:])


def solution(mesh):
    placed = (P("seq", "head"), P("seq", None), P("seq", None), P("seq", "head"))
    return jax.shard_map(
        local,
        mesh=mesh,
        in_specs=placed,
        out_specs=(P("seq", "head"), P("seq", "head"), P("seq", None), P("seq", None)),
        check_vma=False,
    )
```

```python
import functools

import jax
import jax.numpy as jnp
from jax import lax
from jax.experimental import pallas as pl
from jax.experimental.pallas import tpu as pltpu
from jax.sharding import PartitionSpec as P

EPSILON = 1e-06
VMEM_LIMIT = 16 * 1024 * 1024


def contract(left, right, left_dim, right_dim):
    return lax.dot_general(
        left, right, (((left_dim,), (right_dim,)), ((), ())), preferred_element_type=jnp.float32
    )


def call(kernel, outs, *operands, name):
    vmem = pl.BlockSpec(memory_space=pltpu.VMEM)
    operands = [pltpu.with_memory_space_constraint(x, pltpu.VMEM) for x in operands]
    return pl.pallas_call(
        kernel,
        out_shape=[pltpu.VMEM(shape, kind) for shape, kind in outs],
        in_specs=[vmem] * len(operands),
        out_specs=[vmem] * len(outs),
        compiler_params=pltpu.CompilerParams(vmem_limit_bytes=VMEM_LIMIT),
        name=name,
    )(*operands)


def load_kernel(query_hbm, key_hbm, value_hbm, grad_hbm, pair_ref, query_ref, grad_ref, sems):
    rows, head_width = key_hbm.shape
    copies = [(key_hbm, pair_ref.at[:, :head_width]), (value_hbm, pair_ref.at[:, head_width:])]
    for h in range(query_hbm.shape[1] // head_width):
        columns, below = pl.ds(h * head_width, head_width), pl.ds(h * rows, rows)
        copies.append((query_hbm.at[:, columns], query_ref.at[below, :]))
        copies.append((grad_hbm.at[:, columns], grad_ref.at[below, :]))
    copies = [
        pltpu.make_async_copy(source, target, sems.at[i])
        for i, (source, target) in enumerate(copies)
    ]
    for copy in copies:
        copy.start()
    for copy in copies:
        copy.wait()


def load(query_rows, key_rows, value_rows, out_grad):
    rows, head_width = key_rows.shape
    heads = query_rows.shape[1] // head_width
    stack = pltpu.VMEM((heads * rows, head_width), query_rows.dtype)
    operands = [
        pltpu.with_memory_space_constraint(x, pltpu.HBM)
        for x in (query_rows, key_rows, value_rows, out_grad)
    ]
    return pl.pallas_call(
        load_kernel,
        out_shape=[pltpu.VMEM((rows, 2 * head_width), key_rows.dtype), stack, stack],
        in_specs=[pl.BlockSpec(memory_space=pltpu.HBM)] * 4,
        out_specs=[pl.BlockSpec(memory_space=pltpu.VMEM)] * 3,
        scratch_shapes=[pltpu.SemaphoreType.DMA((2 + 2 * heads,))],
        compiler_params=pltpu.CompilerParams(vmem_limit_bytes=VMEM_LIMIT),
        name="load",
    )(*operands)


def halves(refs):
    width = refs[0].shape[1] // 2
    return (
        jnp.concatenate([ref[:, :width] for ref in refs], axis=0),
        jnp.concatenate([ref[:, width:] for ref in refs], axis=0),
    )


def forward_kernel(masks, *refs):
    count = len(masks)
    slots, (query_ref, grad_ref) = refs[:count], refs[count : count + 2]
    score_refs, (numer_ref, out_ref) = refs[count + 2 : -2], refs[-2:]
    rows, head_width = slots[0].shape[0], slots[0].shape[1] // 2
    own = lax.axis_index("seq")
    query = query_ref[...]
    columns = query.shape[0]
    numerator = jnp.zeros((head_width, columns), jnp.float32)
    half = count // len(score_refs)
    for i, score_ref in enumerate(score_refs):
        span = slice(i * half, (i + 1) * half)
        keys, values = halves(slots[span])
        score = contract(keys, query, 1, 1)
        pieces = []
        for j, mask in enumerate(masks[span]):
            piece = score[j * rows : (j + 1) * rows, :]
            if mask == 0:
                key_place = lax.broadcasted_iota(jnp.int32, (rows, columns), 0)
                query_place = lax.broadcasted_iota(jnp.int32, (rows, columns), 1) % rows
                piece = jnp.where(key_place <= query_place, piece, 0.0)
            else:
                piece = jnp.where((own ^ mask) < own, piece, 0.0)
            pieces.append(piece)
        score = jnp.concatenate(pieces, axis=0)
        score_ref[...] = score
        numerator = numerator + contract(values, (score * score).astype(jnp.bfloat16), 0, 0)
    numerator = numerator.T
    root_mean = jnp.sqrt(jnp.mean(numerator * numerator, axis=-1, keepdims=True) + EPSILON)
    normed = numerator / root_mean
    grad = grad_ref[...].astype(jnp.float32)
    numer_ref[...] = (
        (grad - normed * jnp.mean(grad * normed, axis=-1, keepdims=True)) / root_mean
    ).astype(jnp.bfloat16)
    attended = normed.astype(jnp.bfloat16)
    for h in range(columns // rows):
        out_ref[:, h * head_width : (h + 1) * head_width] = attended[h * rows : (h + 1) * rows, :]


def backward_kernel(*refs):
    slots, (score_ref, numer_ref, query_ref, coefficient_ref, dkv_ref) = refs[:-5], refs[-5:]
    rows, head_width = slots[0].shape[0], slots[0].shape[1] // 2
    _, values = halves(slots)
    query = query_ref[...]
    numer_grad = numer_ref[...]
    score = score_ref[...]
    coefficient = (2.0 * score * contract(values, numer_grad, 1, 1)).astype(jnp.bfloat16)
    coefficient_ref[...] = coefficient
    dkv_ref[:, :head_width] = contract(coefficient, query, 1, 0).astype(jnp.bfloat16)
    weight = (score * score).astype(jnp.bfloat16)
    dkv_ref[:, head_width:] = contract(weight, numer_grad, 1, 0).astype(jnp.bfloat16)


def query_kernel(*refs):
    slots, coefficient_refs, dquery_ref = refs[:-3], refs[-3:-1], refs[-1]
    rows, head_width = slots[0].shape[0], slots[0].shape[1] // 2
    half = len(slots) // 2
    dquery = 0.0
    for i, coefficient_ref in enumerate(coefficient_refs):
        keys, _ = halves(slots[i * half : (i + 1) * half])
        dquery = dquery + contract(keys, coefficient_ref[...], 0, 0)
    dquery = dquery.T.astype(jnp.bfloat16)
    for h in range(dquery.shape[0] // rows):
        dquery_ref[:, h * head_width : (h + 1) * head_width] = dquery[h * rows : (h + 1) * rows, :]


def partner(array, axis, mask):
    return lax.ppermute(array, axis, [(i, i ^ mask) for i in range(lax.axis_size(axis))])


def local(query_rows, key_rows, value_rows, out_grad):
    rows, head_width = key_rows.shape
    blocks, head_axis = lax.axis_size("seq"), lax.axis_size("head")
    columns = query_rows.shape[1] // head_width * rows
    evens = tuple(range(0, blocks, 2))
    half = rows * len(evens)
    pair, query, grad = load(query_rows, key_rows, value_rows, out_grad)
    even = [pair] + [partner(pair, "seq", m) for m in evens[1:]]
    odd = [partner(block, "seq", 1) for block in even]
    masks = evens + tuple(m ^ 1 for m in evens)
    score_even, score_odd, numer_grad, attended = call(
        functools.partial(forward_kernel, masks),
        [((half, columns), jnp.float32)] * 2
        + [((columns, head_width), jnp.bfloat16), (query_rows.shape, jnp.bfloat16)],
        *even,
        *odd,
        query,
        grad,
        name="forward",
    )
    outs = [((half, columns), jnp.bfloat16), ((half, 2 * head_width), jnp.bfloat16)]
    coefficient_odd, away = call(
        backward_kernel, outs, *odd, score_odd, numer_grad, query, name="backward_odd"
    )
    swapped = partner(away, "seq", 1)
    coefficient_even, kept = call(
        backward_kernel, outs, *even, score_even, numer_grad, query, name="backward_even"
    )
    chip = kept.astype(jnp.float32) + swapped.astype(jnp.float32)
    chip = chip.reshape(len(evens), rows, 2 * head_width)
    summed = chip[0]
    arrived = [
        partner(chip[i].astype(jnp.bfloat16), "seq", evens[i]) for i in range(1, len(evens))
    ]
    for piece in arrived:
        summed = summed + piece.astype(jnp.float32)
    (query_grad,) = call(
        query_kernel,
        [(query_rows.shape, jnp.bfloat16)],
        *even,
        *odd,
        coefficient_even,
        coefficient_odd,
        name="query_grad",
    )
    sent = summed.astype(jnp.bfloat16)
    for mask in range(1, head_axis):
        summed = summed + partner(sent, "head", mask).astype(jnp.float32)
    summed = summed.astype(jnp.bfloat16)
    return (attended, query_grad, summed[:, :head_width], summed[:, head_width:])


def solution(mesh):
    placed = (P("seq", "head"), P("seq", None), P("seq", None), P("seq", "head"))
    return jax.shard_map(
        local,
        mesh=mesh,
        in_specs=placed,
        out_specs=(P("seq", "head"), P("seq", "head"), P("seq", None), P("seq", None)),
        check_vma=False,
    )
```

```python
import functools

import jax
import jax.numpy as jnp
from jax import lax
from jax.experimental import pallas as pl
from jax.experimental.pallas import tpu as pltpu
from jax.sharding import PartitionSpec as P


EPSILON = 1e-06
VMEM_LIMIT = 16 * 1024 * 1024


def contract(left, right, left_dim, right_dim):
    return lax.dot_general(
        left, right, (((left_dim,), (right_dim,)), ((), ())), preferred_element_type=jnp.float32
    )


def call(kernel, outs, *operands, space=pltpu.VMEM, scratch=()):
    return pl.pallas_call(
        kernel,
        out_shape=[pltpu.VMEM(shape, kind) for shape, kind in outs],
        in_specs=[pl.BlockSpec(memory_space=space)] * len(operands),
        out_specs=[pl.BlockSpec(memory_space=pltpu.VMEM)] * len(outs),
        scratch_shapes=scratch,
        compiler_params=pltpu.CompilerParams(vmem_limit_bytes=VMEM_LIMIT),
    )(*[pltpu.with_memory_space_constraint(x, space) for x in operands])


def run(copies, sems):
    copies = [
        pltpu.make_async_copy(source, target, sems.at[i])
        for i, (source, target) in enumerate(copies)
    ]
    for copy in copies:
        copy.start()
    for copy in copies:
        copy.wait()


def load_pair_kernel(key_hbm, value_hbm, pair_ref, sems):
    head_width = key_hbm.shape[1]
    run([(key_hbm, pair_ref.at[:, :head_width]), (value_hbm, pair_ref.at[:, head_width:])], sems)


def load_kernel(query_hbm, grad_hbm, stack_ref, grad_ref, sems):
    rows, head_width = query_hbm.shape[0], stack_ref.shape[1]
    heads = query_hbm.shape[1] // head_width
    copies = [(grad_hbm, grad_ref)]
    for h in range(heads):
        source = query_hbm.at[:, pl.ds(h * head_width, head_width)]
        copies.append((source, stack_ref.at[pl.ds(h * rows, rows), :]))
    run(copies, sems)
    for h in range(heads):
        turned = grad_ref[:, h * head_width : (h + 1) * head_width].T
        below = heads * rows + h * head_width
        stack_ref[below : below + head_width, :] = turned


def halves(refs):
    width = refs[0].shape[1] // 2
    return (
        jnp.concatenate([ref[:, :width] for ref in refs], axis=0),
        jnp.concatenate([ref[:, width:] for ref in refs], axis=0),
    )


def queries(own_ref, other_ref):
    count = own_ref.shape[0] // 2
    return jnp.concatenate([own_ref[:count, :], other_ref[:count, :]], axis=0)


def cotangents(own_ref, other_ref):
    width = own_ref.shape[1]
    count = own_ref.shape[0]
    tiles = [
        ref[at : at + width, :]
        for ref in (own_ref, other_ref)
        for at in range(count // 2, count, width)
    ]
    return jnp.concatenate(tiles, axis=1)


def forward_kernel(masks, *refs):
    slots, (own_ref, other_ref, score_ref, kept_ref, sent_ref) = refs[:-5], refs[-5:]
    rows = slots[0].shape[0]
    own = lax.axis_index("seq")
    query = queries(own_ref, other_ref)
    columns = query.shape[0] // 2
    keys, values = halves(slots)
    score = contract(keys, query, 1, 1)
    pieces = []
    for i, mask in enumerate(masks):
        piece = score[i * rows : (i + 1) * rows, :]
        if mask == 0:
            key_place = lax.broadcasted_iota(jnp.int32, (rows, columns), 0)
            query_place = lax.broadcasted_iota(jnp.int32, (rows, columns), 1) % rows
            here = jnp.where(key_place <= query_place, piece[:, :columns], 0.0)
            there = jnp.where(own < (own ^ 1), piece[:, columns:], 0.0)
            piece = jnp.concatenate([here, there], axis=1)
        else:
            piece = jnp.where((own ^ mask) < own, piece, 0.0)
        pieces.append(piece)
    score = jnp.concatenate(pieces, axis=0)
    score_ref[...] = score
    numerator = contract(values, (score * score).astype(jnp.bfloat16), 0, 0)
    kept_ref[...] = numerator
    sent_ref[:, :columns] = numerator[:, columns:].astype(jnp.bfloat16)
    sent_ref[:, columns:] = numerator[:, :columns].astype(jnp.bfloat16)


def backward_kernel(count, *refs):
    slots, refs = refs[:count], refs[count:]
    score_ref, kept_ref, came_ref, own_ref, other_ref, normed_ref, coefficient_ref = refs[:7]
    dkv_refs = refs[7:]
    rows, head_width = slots[0].shape[0], slots[0].shape[1] // 2
    numerator = kept_ref[...] + came_ref[...].astype(jnp.float32)
    root_mean = jnp.sqrt(jnp.mean(numerator * numerator, axis=0, keepdims=True) + EPSILON)
    normed = numerator / root_mean
    grad = cotangents(own_ref, other_ref).astype(jnp.float32)
    numer_grad = (
        (grad - normed * jnp.mean(grad * normed, axis=0, keepdims=True)) / root_mean
    ).astype(jnp.bfloat16)
    _, values = halves(slots)
    score = score_ref[...]
    coefficient = (2.0 * score * contract(values, numer_grad, 1, 0)).astype(jnp.bfloat16)
    weight = (score * score).astype(jnp.bfloat16)
    coefficient_ref[...] = coefficient
    normed_ref[...] = normed[:, : normed_ref.shape[1]].astype(jnp.bfloat16)
    dkey = contract(coefficient, queries(own_ref, other_ref), 1, 0)
    dvalue = contract(weight, numer_grad, 1, 1)
    for i, dkv_ref in enumerate(dkv_refs):
        span = slice(i * rows, (i + 1) * rows)
        dkv_ref[:, :head_width] = dkey[span, :].astype(dkv_ref.dtype)
        dkv_ref[:, head_width:] = dvalue[span, :].astype(dkv_ref.dtype)


def query_kernel(*refs):
    slots, (normed_ref, coefficient_ref, out_ref, kept_ref, sent_ref) = refs[:-5], refs[-5:]
    rows, head_width = slots[0].shape[0], slots[0].shape[1] // 2
    keys, _ = halves(slots)
    dquery = contract(keys, coefficient_ref[...], 0, 0)
    columns = kept_ref.shape[1]
    kept_ref[...] = dquery[:, :columns]
    sent_ref[...] = dquery[:, columns:].astype(jnp.bfloat16)
    for h in range(columns // rows):
        out_ref[:, h * head_width : (h + 1) * head_width] = normed_ref[
            :, h * rows : (h + 1) * rows
        ].T


def query_sum_kernel(kept_ref, came_ref, out_ref):
    rows, head_width = out_ref.shape[0], kept_ref.shape[0]
    total = (kept_ref[...] + came_ref[...].astype(jnp.float32)).astype(jnp.bfloat16)
    for h in range(out_ref.shape[1] // head_width):
        out_ref[:, h * head_width : (h + 1) * head_width] = total[:, h * rows : (h + 1) * rows].T


def partner(array, axis, mask):
    return lax.ppermute(array, axis, [(i, i ^ mask) for i in range(lax.axis_size(axis))])


def shifted(array, axis, step):
    size = lax.axis_size(axis)
    return lax.ppermute(array, axis, [(i, (i + step) % size) for i in range(size)])


def local(query_rows, key_rows, value_rows, out_grad):
    rows, head_width = key_rows.shape
    blocks, head_axis = lax.axis_size("seq"), lax.axis_size("head")
    heads = query_rows.shape[1] // head_width
    columns = heads * rows
    masks = tuple(range(0, blocks, 2))
    half = rows * len(masks)
    low, full = jnp.bfloat16, jnp.float32
    (pair,) = call(
        load_pair_kernel,
        [((rows, 2 * head_width), low)],
        key_rows,
        value_rows,
        space=pltpu.HBM,
        scratch=[pltpu.SemaphoreType.DMA((2,))],
    )
    slots = [pair] + [partner(pair, "seq", m) for m in masks[1:]]
    (own,) = call(
        load_kernel,
        [((heads * (rows + head_width), head_width), low)],
        query_rows,
        out_grad,
        space=pltpu.HBM,
        scratch=[pltpu.VMEM(out_grad.shape, low), pltpu.SemaphoreType.DMA((1 + heads,))],
    )
    other = partner(own, "seq", 1)
    score, kept, sent = call(
        functools.partial(forward_kernel, masks),
        [
            ((half, 2 * columns), full),
            ((head_width, 2 * columns), full),
            ((head_width, 2 * columns), low),
        ],
        *slots,
        own,
        other,
    )
    came = partner(sent, "seq", 1)
    normed, coefficient, summed, *away = call(
        functools.partial(backward_kernel, len(slots)),
        [((head_width, columns), low), ((half, 2 * columns), low), ((rows, 2 * head_width), full)]
        + [((rows, 2 * head_width), low)] * (len(masks) - 1),
        *slots,
        score,
        kept,
        came,
        own,
        other,
    )
    for mask, piece in zip(masks[1:], away):
        summed = summed + partner(piece, "seq", mask).astype(full)
    attended, dquery, dquery_other = call(
        query_kernel,
        [(query_rows.shape, low), ((head_width, columns), full), ((head_width, columns), low)],
        *slots,
        normed,
        coefficient,
    )
    (query_grad,) = call(
        query_sum_kernel, [(query_rows.shape, low)], dquery, partner(dquery_other, "seq", 1)
    )
    sent = summed.astype(low)
    for step in range(1, head_axis):
        summed = summed + shifted(sent, "head", step).astype(full)
    summed = summed.astype(low)
    return (attended, query_grad, summed[:, :head_width], summed[:, head_width:])


def solution(mesh):
    placed = (P("seq", "head"), P("seq", None), P("seq", None), P("seq", "head"))

    return jax.shard_map(
        local,
        mesh=mesh,
        in_specs=placed,
        out_specs=(P("seq", "head"), P("seq", "head"), P("seq", None), P("seq", None)),
        check_vma=False,
    )
```

```python
import functools

import jax
import jax.numpy as jnp
from jax import lax
from jax.experimental import pallas as pl
from jax.experimental.pallas import tpu as pltpu
from jax.sharding import PartitionSpec as P


EPSILON = 1e-06
VMEM_LIMIT = 16 * 1024 * 1024


def contract(left, right, left_dim, right_dim):
    return lax.dot_general(
        left, right, (((left_dim,), (right_dim,)), ((), ())), preferred_element_type=jnp.float32
    )


def call(kernel, outs, *operands, space=pltpu.VMEM, scratch=()):
    return pl.pallas_call(
        kernel,
        out_shape=[pltpu.VMEM(shape, kind) for shape, kind in outs],
        in_specs=[pl.BlockSpec(memory_space=space)] * len(operands),
        out_specs=[pl.BlockSpec(memory_space=pltpu.VMEM)] * len(outs),
        scratch_shapes=scratch,
        compiler_params=pltpu.CompilerParams(vmem_limit_bytes=VMEM_LIMIT),
    )(*[pltpu.with_memory_space_constraint(x, space) for x in operands])


def run(copies, sems):
    copies = [
        pltpu.make_async_copy(source, target, sems.at[i])
        for i, (source, target) in enumerate(copies)
    ]
    for copy in copies:
        copy.start()
    for copy in copies:
        copy.wait()


def load_pair_kernel(key_hbm, value_hbm, pair_ref, sems):
    head_width = key_hbm.shape[1]
    run([(key_hbm, pair_ref.at[:, :head_width]), (value_hbm, pair_ref.at[:, head_width:])], sems)


def load_kernel(query_hbm, grad_hbm, stack_ref, grad_ref, sems):
    rows, head_width = query_hbm.shape[0], stack_ref.shape[1]
    heads = query_hbm.shape[1] // head_width
    copies = [(grad_hbm, grad_ref)]
    for h in range(heads):
        source = query_hbm.at[:, pl.ds(h * head_width, head_width)]
        copies.append((source, stack_ref.at[pl.ds(h * rows, rows), :]))
    run(copies, sems)
    for h in range(heads):
        turned = grad_ref[:, h * head_width : (h + 1) * head_width].T
        below = heads * rows + h * head_width
        stack_ref[below : below + head_width, :] = turned


def halves(refs):
    width = refs[0].shape[1] // 2
    return (
        jnp.concatenate([ref[:, :width] for ref in refs], axis=0),
        jnp.concatenate([ref[:, width:] for ref in refs], axis=0),
    )


def queries(own_ref, other_ref):
    count = own_ref.shape[0] // 2
    return jnp.concatenate([own_ref[:count, :], other_ref[:count, :]], axis=0)


def cotangents(own_ref, other_ref):
    width = own_ref.shape[1]
    count = own_ref.shape[0]
    tiles = [
        ref[at : at + width, :]
        for ref in (own_ref, other_ref)
        for at in range(count // 2, count, width)
    ]
    return jnp.concatenate(tiles, axis=1)


def forward_kernel(masks, *refs):
    slots, refs = refs[: len(masks)], refs[len(masks) :]
    own_ref, other_ref, score_ref, weight_ref, kept_ref, sent_ref = refs
    rows = slots[0].shape[0]
    own = lax.axis_index("seq")
    query = queries(own_ref, other_ref)
    columns = query.shape[0] // 2
    keys, values = halves(slots)
    earlier = [
        jnp.where((own ^ mask) < own, keys[i * rows : (i + 1) * rows, :], 0.0).astype(keys.dtype)
        for i, mask in enumerate(masks)
        if mask
    ]
    score = contract(jnp.concatenate([keys[:rows, :], *earlier], axis=0), query, 1, 1)
    key_place = lax.broadcasted_iota(jnp.int32, (rows, columns), 0)
    query_place = lax.broadcasted_iota(jnp.int32, (rows, columns), 1) % rows
    here = jnp.where(key_place <= query_place, score[:rows, :columns], 0.0)
    there = jnp.where(own < (own ^ 1), score[:rows, columns:], 0.0)
    score = jnp.concatenate([jnp.concatenate([here, there], axis=1), score[rows:, :]], axis=0)
    weight = (score * score).astype(jnp.bfloat16)
    score_ref[...] = score
    weight_ref[...] = weight
    numerator = contract(values, weight, 0, 0)
    kept_ref[...] = numerator
    sent_ref[:, :columns] = numerator[:, columns:].astype(jnp.bfloat16)
    sent_ref[:, columns:] = numerator[:, :columns].astype(jnp.bfloat16)


def key_side(values, score, weight, query, numer_grad):
    coefficient = (score * contract(values, numer_grad, 1, 0)).astype(jnp.bfloat16)
    dkey = 2.0 * contract(coefficient, query, 1, 0)
    return coefficient, jnp.concatenate([dkey, contract(weight, numer_grad, 1, 1)], axis=1)


def away_kernel(count, *refs):
    slots, refs = refs[:count], refs[count:]
    score_ref, weight_ref, kept_ref, came_ref, own_ref, other_ref = refs[:6]
    normed_ref, numer_ref, coefficient_ref = refs[6:9]
    rows = slots[0].shape[0]
    numerator = kept_ref[...] + came_ref[...].astype(jnp.float32)
    inverse = 1.0 / jnp.sqrt(jnp.mean(numerator * numerator, axis=0, keepdims=True) + EPSILON)
    normed = numerator * inverse
    grad = cotangents(own_ref, other_ref).astype(jnp.float32)
    numer_grad = (
        (grad - normed * jnp.mean(grad * normed, axis=0, keepdims=True)) * inverse
    ).astype(jnp.bfloat16)
    _, values = halves(slots)
    coefficient, dkv = key_side(
        values,
        score_ref[rows:, :],
        weight_ref[rows:, :],
        queries(own_ref, other_ref),
        numer_grad,
    )
    dkv = dkv.astype(jnp.bfloat16)
    for i, dkv_ref in enumerate(refs[9:]):
        dkv_ref[...] = dkv[i * rows : (i + 1) * rows, :]
    coefficient_ref[...] = coefficient
    numer_ref[...] = numer_grad
    normed_ref[...] = normed[:, : normed_ref.shape[1]].astype(jnp.bfloat16)


def home_kernel(*refs):
    slots, refs = refs[:-11], refs[-11:]
    score_ref, weight_ref, own_ref, other_ref, numer_ref, coefficient_ref, normed_ref = refs[:7]
    dkv_ref, out_ref, kept_ref, sent_ref = refs[7:]
    rows, head_width = slots[0].shape[0], slots[0].shape[1] // 2
    keys, values = halves(slots)
    coefficient, dkv_ref[...] = key_side(
        values[:rows, :],
        score_ref[:rows, :],
        weight_ref[:rows, :],
        queries(own_ref, other_ref),
        numer_ref[...],
    )
    coefficient = jnp.concatenate([coefficient, coefficient_ref[...]], axis=0)
    dquery = 2.0 * contract(keys, coefficient, 0, 0)
    columns = kept_ref.shape[1]
    kept_ref[...] = dquery[:, :columns]
    sent_ref[...] = dquery[:, columns:].astype(jnp.bfloat16)
    for h in range(columns // rows):
        out_ref[:, h * head_width : (h + 1) * head_width] = normed_ref[
            :, h * rows : (h + 1) * rows
        ].T


def query_sum_kernel(kept_ref, came_ref, out_ref):
    rows, head_width = out_ref.shape[0], kept_ref.shape[0]
    total = (kept_ref[...] + came_ref[...].astype(jnp.float32)).astype(jnp.bfloat16)
    for h in range(out_ref.shape[1] // head_width):
        out_ref[:, h * head_width : (h + 1) * head_width] = total[:, h * rows : (h + 1) * rows].T


def partner(array, axis, mask):
    return lax.ppermute(array, axis, [(i, i ^ mask) for i in range(lax.axis_size(axis))])


def shifted(array, axis, step):
    size = lax.axis_size(axis)
    return lax.ppermute(array, axis, [(i, (i + step) % size) for i in range(size)])


def local(query_rows, key_rows, value_rows, out_grad):
    rows, head_width = key_rows.shape
    blocks, head_axis = lax.axis_size("seq"), lax.axis_size("head")
    heads = query_rows.shape[1] // head_width
    columns = heads * rows
    masks = tuple(range(0, blocks, 2))
    half = rows * len(masks)
    low, full = jnp.bfloat16, jnp.float32
    (pair,) = call(
        load_pair_kernel,
        [((rows, 2 * head_width), low)],
        key_rows,
        value_rows,
        space=pltpu.HBM,
        scratch=[pltpu.SemaphoreType.DMA((2,))],
    )
    slots = [pair] + [partner(pair, "seq", m) for m in masks[1:]]
    (own,) = call(
        load_kernel,
        [((heads * (rows + head_width), head_width), low)],
        query_rows,
        out_grad,
        space=pltpu.HBM,
        scratch=[pltpu.VMEM(out_grad.shape, low), pltpu.SemaphoreType.DMA((1 + heads,))],
    )
    other = partner(own, "seq", 1)
    score, weight, kept, sent = call(
        functools.partial(forward_kernel, masks),
        [
            ((half, 2 * columns), full),
            ((half, 2 * columns), low),
            ((head_width, 2 * columns), full),
            ((head_width, 2 * columns), low),
        ],
        *slots,
        own,
        other,
    )
    came = partner(sent, "seq", 1)
    normed, numer_grad, coefficient, *away = call(
        functools.partial(away_kernel, len(slots) - 1),
        [
            ((head_width, columns), low),
            ((head_width, 2 * columns), low),
            ((half - rows, 2 * columns), low),
        ]
        + [((rows, 2 * head_width), low)] * (len(masks) - 1),
        *slots[1:],
        score,
        weight,
        kept,
        came,
        own,
        other,
    )
    arrived = [partner(piece, "seq", m) for m, piece in zip(masks[1:], away)]
    summed, attended, dquery, dquery_other = call(
        home_kernel,
        [
            ((rows, 2 * head_width), full),
            (query_rows.shape, low),
            ((head_width, columns), full),
            ((head_width, columns), low),
        ],
        *slots,
        score,
        weight,
        own,
        other,
        numer_grad,
        coefficient,
        normed,
    )
    for piece in arrived:
        summed = summed + piece.astype(full)
    (query_grad,) = call(
        query_sum_kernel, [(query_rows.shape, low)], dquery, partner(dquery_other, "seq", 1)
    )
    sent = summed.astype(low)
    for step in range(1, head_axis):
        summed = summed + shifted(sent, "head", step).astype(full)
    summed = summed.astype(low)
    return (attended, query_grad, summed[:, :head_width], summed[:, head_width:])


def solution(mesh):
    placed = (P("seq", "head"), P("seq", None), P("seq", None), P("seq", "head"))

    return jax.shard_map(
        local,
        mesh=mesh,
        in_specs=placed,
        out_specs=(P("seq", "head"), P("seq", "head"), P("seq", None), P("seq", None)),
        check_vma=False,
    )
```

```python
import functools

import jax
import jax.numpy as jnp
from jax import lax
from jax.experimental import pallas as pl
from jax.experimental.pallas import tpu as pltpu
from jax.sharding import PartitionSpec as P


EPSILON = 1e-06
VMEM_LIMIT = 16 * 1024 * 1024


def contract(left, right, left_dim, right_dim):
    return lax.dot_general(
        left, right, (((left_dim,), (right_dim,)), ((), ())), preferred_element_type=jnp.float32
    )


def call(kernel, outs, *operands, space=pltpu.VMEM, scratch=()):
    return pl.pallas_call(
        kernel,
        out_shape=[pltpu.VMEM(shape, kind) for shape, kind in outs],
        in_specs=[pl.BlockSpec(memory_space=space)] * len(operands),
        out_specs=[pl.BlockSpec(memory_space=pltpu.VMEM)] * len(outs),
        scratch_shapes=scratch,
        compiler_params=pltpu.CompilerParams(vmem_limit_bytes=VMEM_LIMIT),
    )(*[pltpu.with_memory_space_constraint(x, space) for x in operands])


def run(copies, sems):
    copies = [
        pltpu.make_async_copy(source, target, sems.at[i])
        for i, (source, target) in enumerate(copies)
    ]
    for copy in copies:
        copy.start()
    for copy in copies:
        copy.wait()


def load_pair_kernel(key_hbm, value_hbm, pair_ref, sems):
    head_width = key_hbm.shape[1]
    run([(key_hbm, pair_ref.at[:, :head_width]), (value_hbm, pair_ref.at[:, head_width:])], sems)


def load_kernel(query_hbm, grad_hbm, stack_ref, grad_ref, sems):
    rows, head_width = query_hbm.shape[0], stack_ref.shape[1]
    heads = query_hbm.shape[1] // head_width
    copies = [(grad_hbm, grad_ref)]
    for h in range(heads):
        source = query_hbm.at[:, pl.ds(h * head_width, head_width)]
        copies.append((source, stack_ref.at[pl.ds(h * rows, rows), :]))
    run(copies, sems)
    for h in range(heads):
        turned = grad_ref[:, h * head_width : (h + 1) * head_width].T
        below = heads * rows + h * head_width
        stack_ref[below : below + head_width, :] = turned


def halves(refs):
    width = refs[0].shape[1] // 2
    return (
        jnp.concatenate([ref[:, :width] for ref in refs], axis=0),
        jnp.concatenate([ref[:, width:] for ref in refs], axis=0),
    )


def queries(own_ref, other_ref):
    count = own_ref.shape[0] // 2
    return jnp.concatenate([own_ref[:count, :], other_ref[:count, :]], axis=0)


def cotangents(own_ref, other_ref):
    width = own_ref.shape[1]
    count = own_ref.shape[0]
    tiles = [
        ref[at : at + width, :]
        for ref in (own_ref, other_ref)
        for at in range(count // 2, count, width)
    ]
    return jnp.concatenate(tiles, axis=1)


def forward_kernel(masks, *refs):
    slots, refs = refs[: len(masks)], refs[len(masks) :]
    own_ref, other_ref, score_ref, weight_ref, kept_ref, sent_ref = refs
    rows = slots[0].shape[0]
    own = lax.axis_index("seq")
    query = queries(own_ref, other_ref)
    columns = query.shape[0] // 2
    keys, values = halves(slots)
    earlier = [
        jnp.where((own ^ mask) < own, keys[i * rows : (i + 1) * rows, :], 0.0).astype(keys.dtype)
        for i, mask in enumerate(masks)
        if mask
    ]
    score = contract(jnp.concatenate([keys[:rows, :], *earlier], axis=0), query, 1, 1)
    key_place = lax.broadcasted_iota(jnp.int32, (rows, columns), 0)
    query_place = lax.broadcasted_iota(jnp.int32, (rows, columns), 1) % rows
    here = jnp.where(key_place <= query_place, score[:rows, :columns], 0.0)
    there = jnp.where(own < (own ^ 1), score[:rows, columns:], 0.0)
    score = jnp.concatenate([jnp.concatenate([here, there], axis=1), score[rows:, :]], axis=0)
    weight = (score * score).astype(jnp.bfloat16)
    score_ref[...] = score
    weight_ref[...] = weight
    numerator = contract(values, weight, 0, 0)
    kept_ref[...] = numerator
    sent_ref[:, :columns] = numerator[:, columns:].astype(jnp.bfloat16)
    sent_ref[:, columns:] = numerator[:, :columns].astype(jnp.bfloat16)


def key_side(values, score, weight, query, numer_grad):
    coefficient = (score * contract(values, numer_grad, 1, 0)).astype(jnp.bfloat16)
    dkey = 2.0 * contract(coefficient, query, 1, 0)
    return coefficient, jnp.concatenate([dkey, contract(weight, numer_grad, 1, 1)], axis=1)


def away_kernel(count, *refs):
    slots, refs = refs[:count], refs[count:]
    score_ref, weight_ref, kept_ref, came_ref, own_ref, other_ref = refs[:6]
    normed_ref, numer_ref, coefficient_ref = refs[6:9]
    rows = slots[0].shape[0]
    numerator = kept_ref[...] + came_ref[...].astype(jnp.float32)
    inverse = 1.0 / jnp.sqrt(jnp.mean(numerator * numerator, axis=0, keepdims=True) + EPSILON)
    normed = numerator * inverse
    grad = cotangents(own_ref, other_ref).astype(jnp.float32)
    numer_grad = (
        (grad - normed * jnp.mean(grad * normed, axis=0, keepdims=True)) * inverse
    ).astype(jnp.bfloat16)
    _, values = halves(slots)
    coefficient, dkv = key_side(
        values,
        score_ref[rows:, :],
        weight_ref[rows:, :],
        queries(own_ref, other_ref),
        numer_grad,
    )
    dkv = dkv.astype(jnp.bfloat16)
    for i, dkv_ref in enumerate(refs[9:]):
        dkv_ref[...] = dkv[i * rows : (i + 1) * rows, :]
    coefficient_ref[...] = coefficient
    numer_ref[...] = numer_grad
    normed_ref[...] = normed[:, : normed_ref.shape[1]].astype(jnp.bfloat16)


def home_kernel(*refs):
    slots, refs = refs[:-11], refs[-11:]
    score_ref, weight_ref, own_ref, other_ref, numer_ref, coefficient_ref, normed_ref = refs[:7]
    dkv_ref, out_ref, kept_ref, sent_ref = refs[7:]
    rows, head_width = slots[0].shape[0], slots[0].shape[1] // 2
    keys, values = halves(slots)
    coefficient, dkv_ref[...] = key_side(
        values[:rows, :],
        score_ref[:rows, :],
        weight_ref[:rows, :],
        queries(own_ref, other_ref),
        numer_ref[...],
    )
    coefficient = jnp.concatenate([coefficient, coefficient_ref[...]], axis=0)
    dquery = 2.0 * contract(keys, coefficient, 0, 0)
    columns = kept_ref.shape[1]
    kept_ref[...] = dquery[:, :columns]
    sent_ref[...] = dquery[:, columns:].astype(jnp.bfloat16)
    for h in range(columns // rows):
        out_ref[:, h * head_width : (h + 1) * head_width] = normed_ref[
            :, h * rows : (h + 1) * rows
        ].T


def query_sum_kernel(kept_ref, came_ref, out_ref):
    rows, head_width = out_ref.shape[0], kept_ref.shape[0]
    total = (kept_ref[...] + came_ref[...].astype(jnp.float32)).astype(jnp.bfloat16)
    for h in range(out_ref.shape[1] // head_width):
        out_ref[:, h * head_width : (h + 1) * head_width] = total[:, h * rows : (h + 1) * rows].T


def final_kernel(*refs):
    parts, (key_hbm, value_hbm, key_ref, value_ref, sems) = refs[:-5], refs[-5:]
    width = key_ref.shape[1]
    copies = []
    for i, (target, ref) in enumerate(((key_hbm, key_ref), (value_hbm, value_ref))):
        columns = slice(i * width, (i + 1) * width)
        total = parts[0][:, columns]
        for part in parts[1:]:
            total = total + part[:, columns].astype(jnp.float32)
        ref[...] = total.astype(ref.dtype)
        copies.append(pltpu.make_async_copy(ref, target, sems.at[i]))
        copies[-1].start()
    for copy in copies:
        copy.wait()


def partner(array, axis, mask):
    return lax.ppermute(array, axis, [(i, i ^ mask) for i in range(lax.axis_size(axis))])


def shifted(array, axis, step):
    size = lax.axis_size(axis)
    return lax.ppermute(array, axis, [(i, (i + step) % size) for i in range(size)])


def local(query_rows, key_rows, value_rows, out_grad):
    rows, head_width = key_rows.shape
    blocks, head_axis = lax.axis_size("seq"), lax.axis_size("head")
    heads = query_rows.shape[1] // head_width
    columns = heads * rows
    masks = tuple(range(0, blocks, 2))
    half = rows * len(masks)
    low, full = jnp.bfloat16, jnp.float32
    (pair,) = call(
        load_pair_kernel,
        [((rows, 2 * head_width), low)],
        key_rows,
        value_rows,
        space=pltpu.HBM,
        scratch=[pltpu.SemaphoreType.DMA((2,))],
    )
    slots = [pair] + [partner(pair, "seq", m) for m in masks[1:]]
    (own,) = call(
        load_kernel,
        [((heads * (rows + head_width), head_width), low)],
        query_rows,
        out_grad,
        space=pltpu.HBM,
        scratch=[pltpu.VMEM(out_grad.shape, low), pltpu.SemaphoreType.DMA((1 + heads,))],
    )
    other = partner(own, "seq", 1)
    score, weight, kept, sent = call(
        functools.partial(forward_kernel, masks),
        [
            ((half, 2 * columns), full),
            ((half, 2 * columns), low),
            ((head_width, 2 * columns), full),
            ((head_width, 2 * columns), low),
        ],
        *slots,
        own,
        other,
    )
    came = partner(sent, "seq", 1)
    normed, numer_grad, coefficient, *away = call(
        functools.partial(away_kernel, len(slots) - 1),
        [
            ((head_width, columns), low),
            ((head_width, 2 * columns), low),
            ((half - rows, 2 * columns), low),
        ]
        + [((rows, 2 * head_width), low)] * (len(masks) - 1),
        *slots[1:],
        score,
        weight,
        kept,
        came,
        own,
        other,
    )
    arrived = [partner(piece, "seq", m) for m, piece in zip(masks[1:], away)]
    summed, attended, dquery, dquery_other = call(
        home_kernel,
        [
            ((rows, 2 * head_width), full),
            (query_rows.shape, low),
            ((head_width, columns), full),
            ((head_width, columns), low),
        ],
        *slots,
        score,
        weight,
        own,
        other,
        numer_grad,
        coefficient,
        normed,
    )
    for piece in arrived:
        summed = summed + piece.astype(full)
    (query_grad,) = call(
        query_sum_kernel, [(query_rows.shape, low)], dquery, partner(dquery_other, "seq", 1)
    )
    sent = summed.astype(low)
    pieces = [shifted(sent, "head", step) for step in range(1, head_axis)]
    key_grad, value_grad = pl.pallas_call(
        final_kernel,
        out_shape=[jax.ShapeDtypeStruct(x.shape, low) for x in (key_rows, value_rows)],
        in_specs=[pl.BlockSpec(memory_space=pltpu.VMEM)] * (1 + len(pieces)),
        out_specs=[pl.BlockSpec(memory_space=pltpu.HBM)] * 2,
        scratch_shapes=[pltpu.VMEM(x.shape, low) for x in (key_rows, value_rows)]
        + [pltpu.SemaphoreType.DMA((2,))],
        compiler_params=pltpu.CompilerParams(vmem_limit_bytes=VMEM_LIMIT),
        name="final",
    )(*[pltpu.with_memory_space_constraint(x, pltpu.VMEM) for x in (summed, *pieces)])
    return (attended, query_grad, key_grad, value_grad)


def solution(mesh):
    placed = (P("seq", "head"), P("seq", None), P("seq", None), P("seq", "head"))

    return jax.shard_map(
        local,
        mesh=mesh,
        in_specs=placed,
        out_specs=(P("seq", "head"), P("seq", "head"), P("seq", None), P("seq", None)),
        check_vma=False,
    )
```
